32 devices in a mesh: rep: 8 (over z, core), tp: 4 (over y, x).
Axes of the slice: x: 2, y: 2, z: 4, core: 2. Of those that a mesh axis runs over, the one named last changes fastest.
Arguments:
- delta_query: bfloat16 [8, 2, 2048, 3072], P('rep', None, None, 'tp'), may hold values from -6 to 6
- master_query: float32 [2, 2048, 3072], P(None, 'rep', 'tp'), may hold values from -3 to 3
- moment_query: float32 [2, 2048, 3072], P(None, 'rep', 'tp'), may hold values from -3 to 3
- delta_latent: bfloat16 [8, 2, 512, 4096], P('rep', None, None, 'tp'), may hold values from -6 to 6
- master_latent: float32 [2, 512, 4096], P(None, 'rep', 'tp'), may hold values from -3 to 3
- moment_latent: float32 [2, 512, 4096], P(None, 'rep', 'tp'), may hold values from -3 to 3
- delta_output: bfloat16 [8, 2, 2048, 2048], P('rep', None, 'tp'), may hold values from -6 to 6
- master_output: float32 [2, 2048, 2048], P(None, 'tp', 'rep'), may hold values from -3 to 3
- moment_output: float32 [2, 2048, 2048], P(None, 'tp', 'rep'), may hold values from -3 to 3
Outputs:
- params_query: bfloat16 [2, 2048, 3072], P(None, None, 'tp')
- new_master_query: float32 [2, 2048, 3072], P(None, 'rep', 'tp')
- new_moment_query: float32 [2, 2048, 3072], P(None, 'rep', 'tp')
- params_latent: bfloat16 [2, 512, 4096], P(None, None, 'tp')
- new_master_latent: float32 [2, 512, 4096], P(None, 'rep', 'tp')
- new_moment_latent: float32 [2, 512, 4096], P(None, 'rep', 'tp')
- params_output: bfloat16 [2, 2048, 2048], P(None, 'tp')
- new_master_output: float32 [2, 2048, 2048], P(None, 'tp', 'rep')
- new_moment_output: float32 [2, 2048, 2048], P(None, 'tp', 'rep')
The draws below stay inside these ranges and needn't reach their ends.
All inputs are finite; a program needn't handle non-finite values.
Results may differ from the reference program's by a relative error of at most 0.012.
Values may be sent and summed in bfloat16 or wider, within the bound.
No kernel may reach another device: no remote copies, remote signals or barrier semaphores. Data moves between devices by JAX's collectives and lax.ppermute only.
A program may use at most 128 MiB of HBM per device.

```python
import jax
import jax.numpy as jnp
from jax import lax

D = 2048
KV_RANK = 512
LAYERS = 2
REPLICAS = 8
QCOLS = 3072
KVCOLS = 4096
OROWS = 2048


def spiked(drawn, rng, source, target, blocks, factor):
    owner, partner = [(jnp.arange(drawn.shape[dim]) // (drawn.shape[dim] // blocks)).reshape([-1 if axis == dim else 1 for axis in range(drawn.ndim)]) for dim in (source, target)]
    chosen = jax.random.permutation(rng, blocks)[partner]
    strong = (owner == chosen) | (owner == (partner + blocks // 2) % blocks)
    return jnp.where(strong, factor * drawn, drawn)


def level_of(own_key, dims, pieces, smallest, top_value):
    loudness = 1.0
    for dim, parts in pieces:
        steps = jax.random.uniform(jax.random.fold_in(jax.random.fold_in(own_key, 6), dim), (parts,), jnp.float32, smallest / len(pieces), top_value / len(pieces))
        loudness = loudness * jnp.repeat(jnp.exp(steps), dims[dim] // parts).reshape((-1,) + (1,) * (len(dims) - 1 - dim))
    return loudness


def gaussian(own_key, extent, scale, bound, shards=(), kind=jnp.bfloat16):
    drawn = jax.random.normal(own_key, extent, jnp.float32) * scale
    if len(shards) > 0:
        drawn = level_of(own_key, extent, shards, -0.22, 0.18) * drawn
    return jnp.clip(drawn, min=-bound, max=bound).astype(kind)


def noise_with(rng, dims, deviation, limit, shards, heavy, held_as=jnp.bfloat16):
    entries = deviation * jax.random.normal(rng, dims, jnp.float32)
    if shards:
        entries = entries * level_of(rng, dims, shards, -0.22, 0.18)
    return jnp.clip(spiked(entries, jax.random.fold_in(rng, 3), *heavy), -limit, limit).astype(held_as)


def setup_inputs(seed: int = 0) -> dict:
    streams_of = jax.random.split(jax.random.key(seed), 10)
    delta_query = noise_with(streams_of[0], (REPLICAS, LAYERS, D, QCOLS), 1.0, 6.0, ((0, 8), (3, 4)), (0, 2, 8, 2.0))
    master_query = gaussian(streams_of[1], (LAYERS, D, QCOLS), 0.5, 3.0, ((1, 8), (2, 4)), jnp.float32)
    moment_query = gaussian(streams_of[2], (LAYERS, D, QCOLS), 0.3, 3.0, ((1, 8), (2, 4)), jnp.float32)
    delta_latent = noise_with(streams_of[3], (REPLICAS, LAYERS, KV_RANK, KVCOLS), 1.0, 6.0, ((0, 8), (3, 4)), (0, 2, 8, 2.0))
    master_latent = gaussian(streams_of[4], (LAYERS, KV_RANK, KVCOLS), 0.5, 3.0, ((1, 8), (2, 4)), jnp.float32)
    moment_latent = gaussian(streams_of[5], (LAYERS, KV_RANK, KVCOLS), 0.3, 3.0, ((1, 8), (2, 4)), jnp.float32)
    delta_output = noise_with(streams_of[6], (REPLICAS, LAYERS, OROWS, D), 1.0, 6.0, ((0, 8), (2, 4)), (0, 3, 8, 2.0))
    master_output = gaussian(streams_of[7], (LAYERS, OROWS, D), 0.5, 3.0, ((1, 4), (2, 8)), jnp.float32)
    moment_output = gaussian(streams_of[8], (LAYERS, OROWS, D), 0.3, 3.0, ((1, 4), (2, 8)), jnp.float32)
    return dict(delta_query=delta_query, master_query=master_query, moment_query=moment_query, delta_latent=delta_latent, master_latent=master_latent, moment_latent=moment_latent, delta_output=delta_output, master_output=master_output, moment_output=moment_output)


OUTER_RATE = 0.7
OUTER_MOMENTUM = 0.9


def accumulate(delta):
    def add_replica(replica, running):
        return running + delta[replica].astype(jnp.float32)

    return lax.fori_loop(0, REPLICAS, add_replica, jnp.zeros(delta.shape[1:], jnp.float32))


def update(delta, master, moment):
    average = accumulate(delta) / REPLICAS
    momentum = OUTER_MOMENTUM * moment + average
    updated = master - OUTER_RATE * (average + OUTER_MOMENTUM * momentum)
    return updated.astype(jnp.bfloat16), updated, momentum


def reference(delta_query, master_query, moment_query, delta_latent, master_latent, moment_latent, delta_output, master_output, moment_output):
    query_params, query_master, query_moment = update(delta_query, master_query, moment_query)
    latent_params, latent_master, latent_moment = update(delta_latent, master_latent, moment_latent)
    output_params, output_master, output_moment = update(delta_output, master_output, moment_output)
    return (query_params, query_master, query_moment, latent_params, latent_master, latent_moment, output_params, output_master, output_moment)
```

```python
import functools

import jax
import jax.numpy as jnp
from jax import lax
from jax.experimental import pallas as pl
from jax.experimental.pallas import tpu as pltpu
from jax.sharding import PartitionSpec as P


OUTER_RATE = 0.7
OUTER_MOMENTUM = 0.9
CORES = 2


def nesterov(totals, master, moment, replica_count):
    average = totals / replica_count
    momentum = OUTER_MOMENTUM * moment + average
    updated = master - OUTER_RATE * (average + OUTER_MOMENTUM * momentum)
    return (updated, momentum)


def pack_body(place, kept_in, sent_in, kept, sent):
    kept[0] = kept_in[...]
    sent[0] = sent_in[...]


def pack(place, delta, axis, chips, first, count):
    chunk = list(delta.shape)
    chunk[0] = count
    chunk[axis] //= chips * CORES

    def source(flip):
        def index(step, place):
            core = place[1] if not flip else 1 - place[1]
            where = [first // count, 0, 0]
            where[axis] = ((place[0] + step) % chips) * CORES + core
            return tuple(where)

        return index

    shape = jax.ShapeDtypeStruct((chips, *chunk), delta.dtype)
    out = pl.BlockSpec((1, *chunk), lambda step, place: (step, 0, 0, 0))
    return pl.pallas_call(
        pack_body,
        grid_spec=pltpu.PrefetchScalarGridSpec(
            num_scalar_prefetch=1,
            grid=(chips,),
            in_specs=[
                pl.BlockSpec(tuple(chunk), source(False)),
                pl.BlockSpec(tuple(chunk), source(True)),
            ],
            out_specs=[out, out],
        ),
        out_shape=[shape, shape],
        name="pack",
    )(place, delta, delta)


def place_body(place, *refs, pieces, axis, chips, width):
    sources, whole, stage, loaded, stored = refs[:-4], *refs[-4:]

    def visit(act):
        for k, (distance, flip, layer, layers) in enumerate(pieces):
            chip = place[0] + distance
            core = 1 - place[1] if flip else place[1]
            slot = chip * CORES + core
            where = [pl.ds(layer, layers), slice(None), slice(None)]
            where[axis] = pl.ds(pl.multiple_of(slot * width, width), width)
            held = stage.at[slot, pl.ds(layer, layers)]
            load = pltpu.make_async_copy(sources[k], held, loaded.at[k])
            store = pltpu.make_async_copy(held, whole.at[tuple(where)], stored.at[k])
            pl.when((chip >= 0) & (chip < chips))(functools.partial(act, load, store))

    def forward(load, store):
        load.wait()
        store.start()

    visit(lambda load, store: load.start())
    visit(forward)
    visit(lambda load, store: store.wait())


def assemble(place, arrays, pieces, axis, chips, shape, dtype):
    width = shape[axis]
    full = list(shape)
    full[axis] = width * chips * CORES
    count = len(arrays)
    return pl.pallas_call(
        functools.partial(place_body, pieces=pieces, axis=axis, chips=chips, width=width),
        in_specs=[pl.BlockSpec(memory_space=pltpu.SMEM)]
        + [pl.BlockSpec(memory_space=pl.ANY)] * count,
        out_specs=pl.BlockSpec(memory_space=pl.ANY),
        out_shape=jax.ShapeDtypeStruct(tuple(full), dtype),
        scratch_shapes=[
            pltpu.VMEM((chips * CORES, *shape), dtype),
            pltpu.SemaphoreType.DMA((count,)),
            pltpu.SemaphoreType.DMA((count,)),
        ],
        name="assemble",
    )(place, *arrays)


def timetable(names, chips):
    steps = [("reduce", d) for d in range(chips - 1, 0, -1)]
    steps += [("gather", d) for d in range(1, chips)]
    offset = max(1, chips // 2)
    order = []
    for slot in range(len(steps) + offset * len(names)):
        for k, name in enumerate(names):
            at = slot - offset * k
            if 0 <= at < len(steps):
                order.append((name, *steps[at]))
    return order


def outer_step(*args):
    matrices = {
        "query": (*args[0:3], 1),
        "latent": (*args[3:6], 1),
        "output": (*args[6:9], 2),
    }
    replicas = lax.axis_size("rep")
    chips = replicas // CORES
    me = lax.axis_index("rep")
    place = jnp.stack([me // CORES, me % CORES]).astype(jnp.int32)
    f32, bf16 = jnp.float32, jnp.bfloat16
    layers = args[0].shape[1]
    groups = {"output": ("output", 0, layers)}
    groups.update({f"query{n}": ("query", n, 1) for n in range(layers)})
    groups["latent"] = ("latent", 0, layers)

    def to_chip(x, step, senders):
        pairs = [
            (q * CORES + c, (q + step) * CORES + c) for q in senders for c in range(CORES)
        ]
        return lax.ppermute(x, "rep", pairs)

    def to_core(x):
        return lax.ppermute(x, "rep", [(r, r ^ 1) for r in range(replicas)])

    kept, got = {}, {}
    for name, (matrix, first, count) in groups.items():
        delta, _, _, axis = matrices[matrix]
        kept[name], sent = pack(place, delta[0], axis, chips, first, count)
        got[name] = to_core(sent)

    def pair_sum(name, distance):
        d = distance % chips
        return kept[name][d].astype(f32) + got[name][d].astype(f32)

    right, left, totals = {}, {}, {}
    pieces = {matrix: [] for matrix in matrices}
    arrays = {matrix: [] for matrix in matrices}

    def keep_piece(name, piece, distance):
        matrix, first, count = groups[name]
        for flip, held in ((False, piece), (True, to_core(piece))):
            arrays[matrix].append(held)
            pieces[matrix].append((distance, flip, first, count))

    for name, kind, d in timetable(list(groups), chips):
        matrix, first, count = groups[name]
        if kind == "reduce":
            a, b = pair_sum(name, d), pair_sum(name, -d)
            if name in right:
                a, b = a + right[name].astype(f32), b + left[name].astype(f32)
            a, b = a.astype(bf16), b.astype(bf16)
            senders = range(chips - d)
        else:
            if d == 1:
                _, master, moment, _ = matrices[matrix]
                total = pair_sum(name, 0)
                if name in right:
                    total = total + right[name].astype(f32) + left[name].astype(f32)
                totals[name] = total
                span = slice(first, first + count)
                updated, _ = nesterov(total, master[span], moment[span], replicas)
                right[name] = left[name] = updated.astype(bf16)
                keep_piece(name, right[name], 0)
            a, b = right[name], left[name]
            senders = range(d - 1, chips - 1)
        right[name] = to_chip(a, 1, senders)
        left[name] = to_chip(b, -1, [chips - 1 - q for q in senders])
        if kind == "gather":
            keep_piece(name, right[name], -d)
            keep_piece(name, left[name], d)

    results = []
    for matrix, (delta, master, moment, axis) in matrices.items():
        parts = [totals[name] for name in groups if groups[name][0] == matrix]
        total = parts[0] if len(parts) == 1 else jnp.concatenate(parts)
        params = assemble(
            place, arrays[matrix], pieces[matrix], axis, chips, master.shape, bf16
        )
        results += [params, *nesterov(total, master, moment, replicas)]
    return tuple(results)


def solution(mesh):
    rows = P(None, "rep", "tp")
    cols = P(None, "tp", "rep")
    by_rows = (P("rep", None, None, "tp"), rows, rows)
    by_cols = (P("rep", None, "tp", None), cols, cols)
    return jax.shard_map(
        outer_step,
        mesh=mesh,
        in_specs=by_rows + by_rows + by_cols,
        out_specs=(
            (P(None, None, "tp"), rows, rows)
            + (P(None, None, "tp"), rows, rows)
            + (P(None, "tp", None), cols, cols)
        ),
        check_vma=False,
    )
```
